16 devices in a mesh: rep: 2 (over y, z), dp: 8 (over x, core).
Axes of the slice: x: 4, y: 2, z: 1, core: 2. Of those that a mesh axis runs over, the one named last changes fastest.
The devices are a block of a 4x4x8 slice.
Arguments:
- a: bfloat16 [16, 4, 4096, 640], P(('rep', 'dp')), parts along dimension 0
- g: bfloat16 [16, 4, 4096, 1536], P(('rep', 'dp')), parts along dimension 0
Outputs:
- output: bfloat16 [8, 640, 1536], P('rep'), parts along dimension 0
There are 2 independent parts. The reference program is written for one: setup_inputs(seed, part) draws one part's arguments, and reference() takes and returns one part's arrays. A program takes and returns all parts, laid end to end along the dimension named above; each array names one.
All inputs are finite; a program needn't handle non-finite values.
Results may differ from the reference program's by a relative error of at most 0.012.
Values are sent between devices in bfloat16 or wider.
A program may use at most 768 MiB of HBM per device.

```python
import jax
import jax.numpy as jnp
from jax import lax

DEVICES = 8
MATRICES = 4
TOKENS = 4096
D = 640
FF = 1536


def setup_inputs(seed: int = 0, part: int = 0) -> dict:
    ka, kg, ks = (jax.random.fold_in(k, part) for k in jax.random.split(jax.random.key(seed), 3))
    size = 2.0 ** jax.random.uniform(ks, (DEVICES, MATRICES, 1, 1), jnp.float32, -1.0, 1.0)
    a = jax.random.normal(ka, (DEVICES, MATRICES, TOKENS, D), jnp.float32)
    g = size * jax.random.normal(kg, (DEVICES, MATRICES, TOKENS, FF), jnp.float32) * (DEVICES * TOKENS) ** -0.5
    return {"a": a.astype(jnp.bfloat16), "g": g.astype(jnp.bfloat16)}


def reference(a, g):
    def take(so_far, one):
        return so_far + jnp.einsum("ntd,ntf->ndf", *one, preferred_element_type=jnp.float32), None

    return lax.scan(take, jnp.zeros((MATRICES, D, FF), jnp.float32), (a, g))[0].astype(jnp.bfloat16)
```

```python
import functools

import jax
import jax.numpy as jnp
from jax import lax
from jax.experimental import pallas as pl
from jax.experimental.pallas import tpu as pltpu
from jax.sharding import PartitionSpec as P

MESH = pl.DeviceIdType.MESH
CORES = 2
NB = 256
KC = 1024
AS = 4
RW = 3
DS = 4


def kernel(
    chips, a_hbm, g_hbm, out, at, a_stage, g_buf, own, d_send, d_recv, r_send, r_recv,
    a_sem, g_sem, ds_sem, dr_sem, rs_sem, rr_sem, fs_sem, fr_sem,
):
    matrices, tokens, d = a_hbm.shape
    ff = g_hbm.shape[2]
    half = d // CORES
    per_matrix = ff // NB
    rounds = matrices * per_matrix // chips
    steps = rounds * chips
    per_wave = RW * chips
    mats_per_wave = per_wave // per_matrix
    blocks = tokens // KC

    me = lax.axis_index("dp")
    chip, core = me // CORES, lax.rem(me, CORES)
    way = 1 - 2 * core
    peer = chip * CORES + 1 - core
    right = lax.rem(chip + way + chips, chips) * CORES + core
    left = lax.rem(chip - way + chips, chips) * CORES + core
    my_rows = pl.ds(pl.multiple_of(core * half, half), half)

    def mine(j):
        return lax.rem(chip - 1 - way * j + chips * chips, chips)

    def peers(j):
        return lax.rem(chip - 1 + way * j + chips * chips, chips)

    def place(r, ch):
        c = r * chips + ch
        return c // per_matrix, pl.ds(pl.multiple_of(lax.rem(c, per_matrix) * NB, NB), NB)

    def load_a(m, b):
        slot = b % AS
        return pltpu.make_async_copy(a_hbm.at[m, pl.ds(b * KC, KC), :], a_stage.at[slot], a_sem.at[slot])

    def load_g(r, ch):
        n, cols = place(r, ch)
        slot = lax.rem(r, RW) * chips + ch
        return pltpu.make_async_copy(g_hbm.at[n, :, cols], g_buf.at[slot], g_sem.at[slot])

    def swap(i):
        return pltpu.make_async_remote_copy(
            src_ref=d_send.at[lax.rem(i, DS)], dst_ref=d_recv.at[i],
            send_sem=ds_sem.at[lax.rem(i, DS)], recv_sem=dr_sem.at[i],
            device_id={"dp": peer}, device_id_type=MESH)

    def reduce_hop(r, j):
        k = r * (chips - 1) + j
        return pltpu.make_async_remote_copy(
            src_ref=r_send.at[k], dst_ref=r_recv.at[k], send_sem=rs_sem.at[r * chips * 2 + j],
            recv_sem=rr_sem.at[r * chips * 2 + j], device_id={"dp": right}, device_id_type=MESH)

    def gather_hop(r, t, ch):
        n, cols = place(r, ch)
        k = r * chips * 2 + chips + t
        return pltpu.make_async_remote_copy(
            src_ref=out.at[n, my_rows, cols], dst_ref=out.at[n, my_rows, cols], send_sem=rs_sem.at[k],
            recv_sem=rr_sem.at[k], device_id={"dp": right}, device_id_type=MESH)

    def hand_over(r, t, ch):
        n, cols = place(r, ch)
        k = r * chips + t
        return pltpu.make_async_remote_copy(
            src_ref=out.at[n, my_rows, cols], dst_ref=out.at[n, my_rows, cols], send_sem=fs_sem.at[k],
            recv_sem=fr_sem.at[k], device_id={"dp": peer}, device_id_type=MESH)

    load_g(0, mine(0)).start()
    for b in range(AS):
        load_a(0, b).start()

    barrier = pltpu.get_barrier_semaphore()
    for other in (left, right, peer):
        pl.semaphore_signal(barrier, inc=1, device_id={"dp": other}, device_id_type=MESH)
    pl.semaphore_wait(barrier, 3)

    def first_loads():
        for j in range(chips):
            for r in range(RW):
                if r or j:
                    load_g(r, lax.rem(chip - 1 + j + chips, chips)).start()

    def transpose(m):
        for b in range(blocks):
            load_a(m, b).wait()
            at[lax.rem(m, mats_per_wave), :, b * KC:(b + 1) * KC] = a_stage[b % AS].T

            @pl.when(m + 1 < matrices)
            def _():
                load_a(m + 1, b).start()

    def combine(i):
        w, ii = i // per_wave, lax.rem(i, per_wave)
        j, r = ii // RW, w * RW + lax.rem(ii, RW)
        swap(i).wait_recv()
        both = own.at[lax.rem(i, 2)]

        @pl.when(j == 0)
        def _():
            r_send[r * (chips - 1)] = (both[...] + d_recv[i].astype(jnp.float32)).astype(jnp.bfloat16)
            reduce_hop(r, 0).start()

        @pl.when(j > 0)
        def _():
            reduce_hop(r, j - 1).wait_recv()
            total = both[...] + d_recv[i].astype(jnp.float32)
            total += r_recv[r * (chips - 1) + j - 1].astype(jnp.float32)
            both[...] = total

        @pl.when((j > 0) & (j < chips - 1))
        def _():
            r_send[r * (chips - 1) + j] = both[...].astype(jnp.bfloat16)
            reduce_hop(r, j).start()

        @pl.when(j == chips - 1)
        def _():
            n, cols = place(r, mine(chips - 1))
            out[n, my_rows, cols] = both[...].astype(jnp.bfloat16)
            gather_hop(r, 0, mine(chips - 1)).start()
            hand_over(r, chips - 1, mine(chips - 1)).start()

    def forward(w, x):
        t, r = x // RW, w * RW + lax.rem(x, RW)
        ch = mine(t)
        gather_hop(r, t, ch).wait_recv()

        @pl.when(t < chips - 2)
        def _():
            gather_hop(r, t + 1, ch).start()

        hand_over(r, t, ch).start()

    def step(i, carry):
        w, ii = i // per_wave, lax.rem(i, per_wave)
        j, r = ii // RW, w * RW + lax.rem(ii, RW)

        @pl.when(ii < mats_per_wave)
        def _():
            transpose(w * mats_per_wave + ii)

        @pl.when(i == 0)
        def _():
            first_loads()

        seen = set()
        for jj in range(chips):
            new = [s for s in {(jj % chips), (-jj) % chips} if s not in seen]
            seen.update(new)
            if new:
                @pl.when(j == jj)
                def _():
                    for s in new:
                        load_g(r, lax.rem(chip - 1 + s + chips, chips)).wait()

        def unit(u, carry):
            ch = jnp.where(u == 0, peers(j), mine(j))
            rows = jnp.where(u == 0, 1 - core, core) * half
            m = (r * chips + ch) // per_matrix
            lhs = at[lax.rem(m, mats_per_wave), pl.ds(pl.multiple_of(rows, half), half), :]
            rhs = g_buf[lax.rem(r, RW) * chips + ch]
            own[jnp.where(u == 0, 2, lax.rem(i, 2))] = jnp.dot(lhs, rhs, preferred_element_type=jnp.float32)

            @pl.when(u == 0)
            def _():
                @pl.when(i >= DS)
                def _():
                    swap(i - DS).wait_send()

                d_send[lax.rem(i, DS)] = own[2].astype(jnp.bfloat16)
                swap(i).start()

                @pl.when(i > 0)
                def _():
                    combine(i - 1)

                @pl.when((w > 0) & (ii < per_wave - RW))
                def _():
                    forward(w - 1, ii)

            return carry

        lax.fori_loop(0, CORES, unit, 0)

        last = {}
        for jj in range(chips):
            for s in {(jj % chips), (-jj) % chips}:
                last[s] = jj
        for jj in range(chips):
            done = [s for s in last if last[s] == jj]
            if done:
                @pl.when((j == jj) & (r + RW < rounds))
                def _():
                    for s in done:
                        load_g(r + RW, lax.rem(chip - 1 + s + chips, chips)).start()

        return carry

    lax.fori_loop(0, steps, step, 0)
    combine(steps - 1)

    waves = steps // per_wave

    def rest(x, carry):
        forward(waves - 1, x)
        return carry

    lax.fori_loop(0, per_wave - RW, rest, 0)

    for i in range(steps - DS, steps):
        swap(i).wait_send()

    def settle(r, carry):
        for j in range(chips - 1):
            reduce_hop(r, j).wait_send()
        for t in range(chips - 1):
            gather_hop(r, t, 0).wait_send()
        for t in range(chips):
            hand_over(r, t, 0).wait()
        return carry

    lax.fori_loop(0, rounds, settle, 0)


def solution(mesh):
    chips = mesh.shape["dp"] // CORES

    def one(a, g):
        a, g = a[0], g[0]
        matrices, tokens, d = a.shape
        ff = g.shape[2]
        half = d // CORES
        steps = matrices * ff // NB
        rounds = steps // chips
        dma = pltpu.SemaphoreType.DMA
        bf16, f32 = jnp.bfloat16, jnp.float32
        return pl.pallas_call(
            functools.partial(kernel, chips),
            out_shape=OUT((matrices, d, ff), bf16) if OUT else jax.ShapeDtypeStruct((matrices, d, ff), bf16),
            in_specs=[pl.BlockSpec(memory_space=pltpu.MemorySpace.HBM)] * 2,
            out_specs=pl.BlockSpec(memory_space=pltpu.MemorySpace.VMEM),
            scratch_shapes=[
                pltpu.VMEM((RW * chips * NB // ff, d, tokens), bf16),
                pltpu.VMEM((AS, KC, d), bf16),
                pltpu.VMEM((RW * chips, tokens, NB), bf16),
                pltpu.VMEM((3, half, NB), f32),
                pltpu.VMEM((DS, half, NB), bf16),
                pltpu.VMEM((steps, half, NB), bf16),
                pltpu.VMEM((rounds * (chips - 1), half, NB), bf16),
                pltpu.VMEM((rounds * (chips - 1), half, NB), bf16),
                dma((AS,)), dma((RW * chips,)), dma((DS,)), dma((steps,)),
                dma((rounds * chips * 2,)), dma((rounds * chips * 2,)), dma((steps,)), dma((steps,)),
            ],
            compiler_params=pltpu.CompilerParams(
                collective_id=0, has_side_effects=True, vmem_limit_bytes=VMEM_LIMIT),
        )(a, g)

    return jax.shard_map(
        one, mesh=mesh, in_specs=(P(("rep", "dp")),) * 2, out_specs=P("rep"), check_vma=False)


OUT = pltpu.MemorySpace.VMEM
VMEM_LIMIT = 53 * 2**20
```

```python
import functools

import jax
import jax.numpy as jnp
from jax import lax
from jax.experimental import pallas as pl
from jax.experimental.pallas import tpu as pltpu
from jax.sharding import PartitionSpec as P

MESH = pl.DeviceIdType.MESH
CORES = 2
NB = 256
AS = 4
AM = 2
RW = 3
DS = 4


def kernel(
    chips, a_hbm, g_hbm, out, at, a_stage, g_buf, whole, own, d_send, d_recv, r_send, r_recv,
    a_sem, h_sem, g_sem, ds_sem, dr_sem, rs_sem, gs_sem, rr_sem, fs_sem, fr_sem,
):
    matrices, tokens, d = a_hbm.shape
    ff = g_hbm.shape[2]
    half = d // CORES
    per_matrix = ff // NB
    rounds = matrices * per_matrix // chips
    steps = rounds * chips
    per_wave = RW * chips
    waves = steps // per_wave
    forwards = per_wave - RW
    block = tokens // AS
    f32, bf16 = jnp.float32, jnp.bfloat16

    me = lax.axis_index("dp")
    chip, core = me // CORES, lax.rem(me, CORES)
    way = 1 - 2 * core
    peer = chip * CORES + 1 - core
    right = lax.rem(chip + way + chips, chips) * CORES + core
    left = lax.rem(chip - way + chips, chips) * CORES + core

    def rows(c):
        return pl.ds(pl.multiple_of(c * half, half), half)

    my_rows, peer_rows = rows(core), rows(1 - core)

    def nth(s):
        return lax.rem(chip - 1 + s + chips * chips, chips)

    def mine(j):
        return nth(-way * j)

    def peers(j):
        return nth(way * j)

    def split(i):
        w, ii = i // per_wave, lax.rem(i, per_wave)
        return ii // RW, w * RW + lax.rem(ii, RW)

    def place(r, ch):
        c = r * chips + ch
        return c // per_matrix, pl.ds(pl.multiple_of(lax.rem(c, per_matrix) * NB, NB), NB)

    def g_slot(r, ch):
        return lax.rem(r, RW) * chips + ch

    def tokens_of(b):
        return pl.ds(pl.multiple_of(b * block, block), block)

    def load_a(m, b):
        return pltpu.make_async_copy(a_hbm.at[m, tokens_of(b), :], a_stage.at[b], a_sem.at[b])

    def load_g(r, ch):
        n, cols = place(r, ch)
        slot = g_slot(r, ch)
        return pltpu.make_async_copy(g_hbm.at[n, :, cols], g_buf.at[slot], g_sem.at[slot])

    def load_first(b):
        n, cols = place(0, nth(0))
        return pltpu.make_async_copy(
            g_hbm.at[n, tokens_of(b), cols], g_buf.at[g_slot(0, nth(0)), tokens_of(b)], h_sem.at[b])

    def to(device, src, dst, send_sem, recv_sem):
        return pltpu.make_async_remote_copy(
            src_ref=src, dst_ref=dst, send_sem=send_sem, recv_sem=recv_sem,
            device_id={"dp": device}, device_id_type=MESH)

    def swap(i):
        s = lax.rem(i, DS)
        return to(peer, d_send.at[s], d_recv.at[s], ds_sem.at[s], dr_sem.at[s])

    def reduce_hop(r, j):
        k = r * (chips - 1) + j
        return to(right, r_send.at[k], r_recv.at[k], rs_sem.at[0], rr_sem.at[r * chips + j])

    def gather_hop(r, t, ch):
        n, cols = place(r, ch)
        at_ = out.at[n, my_rows, cols]
        return to(right, at_, at_, gs_sem.at[0], rr_sem.at[r * chips + lax.rem(t + chips - 1, chips)])

    def hand_over(r, ch):
        n, cols = place(r, ch)
        at_ = out.at[n, my_rows, cols]
        return to(peer, at_, at_, fs_sem.at[0], fr_sem.at[0])

    def transpose(m, b):
        load_a(m, b).wait()
        at[lax.rem(m, AM), :, tokens_of(b)] = a_stage[b].T

        @pl.when(m + 1 < matrices)
        def _():
            load_a(m + 1, b).start()

    def dot(i, ch, which):
        j, r = split(i)
        m = (r * chips + ch) // per_matrix
        return jnp.dot(at[lax.rem(m, AM), which, :], g_buf[g_slot(r, ch)], preferred_element_type=f32)

    def combine(i):
        j, r = split(i)
        s = lax.rem(i, DS)
        swap(i).wait_recv()

        @pl.when(j == 0)
        def _():
            r_send[r * (chips - 1)] = (own[...] + d_recv[s].astype(f32)).astype(bf16)
            reduce_hop(r, 0).start()

        @pl.when(j > 0)
        def _():
            reduce_hop(r, j - 1).wait_recv()
            own[...] = own[...] + d_recv[s].astype(f32) + r_recv[r * (chips - 1) + j - 1].astype(f32)

        @pl.when((j > 0) & (j < chips - 1))
        def _():
            r_send[r * (chips - 1) + j] = own[...].astype(bf16)
            reduce_hop(r, j).start()

        @pl.when(j == chips - 1)
        def _():
            ch = mine(chips - 1)
            n, cols = place(r, ch)
            out[n, my_rows, cols] = own[...].astype(bf16)
            gather_hop(r, 0, ch).start()
            hand_over(r, ch).start()

    def forward(w, x):
        t, r = x // RW, w * RW + lax.rem(x, RW)
        ch = mine(t)
        gather_hop(r, t, ch).wait_recv()

        @pl.when(t < chips - 2)
        def _():
            gather_hop(r, t + 1, ch).start()

        hand_over(r, ch).start()

    def send_peers(i, value):
        d_send[lax.rem(i, DS)] = value.astype(bf16)

    first, last = {}, {}
    for j in range(chips):
        for s in sorted({j, -j % chips}):
            first.setdefault(s, j)
            last[s] = j

    for b in range(AS):
        load_a(0, b).start()
        load_first(b).start()

    barrier = pltpu.get_barrier_semaphore()
    for other in (left, right, peer):
        pl.semaphore_signal(barrier, inc=1, device_id={"dp": other}, device_id_type=MESH)

    always = chip >= 0

    def products(b):
        cols = slice(b * block, (b + 1) * block)
        term = jnp.dot(at[0, :, cols], g_buf[g_slot(0, nth(0)), cols, :], preferred_element_type=f32)
        whole[...] = whole[...] + term if b else term

    for b in range(AS + 1):
        m, k = b // AS, b % AS
        if m == 0:
            load_first(k).wait()
        load_a(m, k).wait()

        @pl.when(always)
        def _():
            at[m, :, k * block:(k + 1) * block] = a_stage[k].T
            if b:
                products(b - 1)

        load_a(m + 1, k).start()
        if 0 < b < RW:
            load_g(b, nth(0)).start()

    send_peers(0, whole[peer_rows, :])
    own[...] = whole[my_rows, :]
    pl.semaphore_wait(barrier, 3)
    swap(0).start()

    for s in sorted(first, key=lambda s: first[s]):
        if s:
            for r in range(RW):
                load_g(r, nth(s)).start()

    for b in range(1, AS):
        transpose(1, b)
        if b == AS - 2:
            combine(0)

    def lone_peers(i, r):
        load_g(r, nth(0)).wait()

        @pl.when(always)
        def _():
            send_peers(i, dot(i, peers(0), peer_rows))

        swap(i).start()

    def lone_mine(i):
        @pl.when(always)
        def _():
            own[...] = dot(i, mine(chips - 1), my_rows)

    def transpose_some(m, begin, end):
        def one(b, carry):
            transpose(m, b)
            return carry

        lax.fori_loop(begin, end, one, 0)

    load_g(RW, nth(0)).start()
    lone_peers(1, 1)

    def step(i, carry):
        w, ii = i // per_wave, lax.rem(i, per_wave)
        j, r = split(i)
        nj, nr = split(i + 1)

        for jj in range(chips):
            new = [s for s in first if first[s] == jj]
            if new:
                @pl.when(nj == jj)
                def _():
                    for s in new:
                        load_g(nr, nth(s)).wait()

        @pl.when(i + 1 >= DS)
        def _():
            swap(i + 1 - DS).wait_send()

        own[...] = dot(i, mine(j), my_rows)
        send_peers(i + 1, dot(i + 1, peers(nj), peer_rows))
        swap(i + 1).start()
        combine(i)

        @pl.when((w > 0) & (ii < forwards - 2))
        def _():
            forward(w - 1, ii + 2)

        for jj in range(chips):
            free = [s for s in last if last[s] == jj]
            if free:
                @pl.when((j == jj) & (r + RW < rounds))
                def _():
                    for s in free:
                        load_g(r + RW, nth(s)).start()

        return carry

    for w in range(waves):
        begin, end = w * per_wave, (w + 1) * per_wave

        if w:
            transpose_some(2 * w, 0, AS)
            forward(w - 1, 0)
            swap(begin - DS).wait_send()
            lone_peers(begin, w * RW)
            transpose_some(2 * w + 1, 0, AS // 2)
            forward(w - 1, 1)
            transpose_some(2 * w + 1, AS // 2, AS)

        lax.fori_loop(begin + (w == 0), end - 1, step, 0)
        lone_mine(end - 1)
        combine(end - 1)
        if w + 1 < waves:
            for q in last:
                if last[q] == chips - 1:
                    load_g((w + 2) * RW - 1, nth(q)).start()

    def rest(x, carry):
        forward(waves - 1, x)
        return carry

    lax.fori_loop(0, forwards, rest, 0)

    for i in range(steps - DS, steps):
        swap(i).wait_send()
    to(right, r_send, r_recv, rs_sem.at[0], rr_sem.at[0]).wait_send()
    to(right, r_send, r_recv, gs_sem.at[0], rr_sem.at[0]).wait_send()
    all_mine = out.at[:, my_rows, :]
    to(peer, all_mine, all_mine, fs_sem.at[0], fr_sem.at[0]).wait()


def solution(mesh):
    chips = mesh.shape["dp"] // CORES

    def one(a, g):
        a, g = a[0], g[0]
        matrices, tokens, d = a.shape
        ff = g.shape[2]
        half = d // CORES
        rounds = matrices * ff // NB // chips
        hops = rounds * (chips - 1)
        bf16, f32 = jnp.bfloat16, jnp.float32
        sems = [AS, AS, RW * chips, DS, DS, 1, 1, rounds * chips, 1, 1]
        return pl.pallas_call(
            functools.partial(kernel, chips),
            out_shape=pltpu.MemorySpace.VMEM((matrices, d, ff), bf16),
            in_specs=[pl.BlockSpec(memory_space=pltpu.MemorySpace.HBM)] * 2,
            out_specs=pl.BlockSpec(memory_space=pltpu.MemorySpace.VMEM),
            scratch_shapes=[
                pltpu.VMEM((AM, d, tokens), bf16),
                pltpu.VMEM((AS, tokens // AS, d), bf16),
                pltpu.VMEM((RW * chips, tokens, NB), bf16),
                pltpu.VMEM((d, NB), f32),
                pltpu.VMEM((half, NB), f32),
                pltpu.VMEM((DS, half, NB), bf16),
                pltpu.VMEM((DS, half, NB), bf16),
                pltpu.VMEM((hops, half, NB), bf16),
                pltpu.VMEM((hops, half, NB), bf16),
                *(pltpu.SemaphoreType.DMA((n,)) for n in sems),
            ],
            compiler_params=pltpu.CompilerParams(
                collective_id=0, has_side_effects=True, vmem_limit_bytes=54 * 2**20),
        )(a, g)

    return jax.shard_map(
        one, mesh=mesh, in_specs=(P(("rep", "dp")),) * 2, out_specs=P("rep"), check_vma=False)
```

```python
import functools

import jax
import jax.numpy as jnp
from jax import lax
from jax.experimental import pallas as pl
from jax.experimental.pallas import tpu as pltpu
from jax.sharding import PartitionSpec as P

MESH = pl.DeviceIdType.MESH
CORES = 2
NB = 256
AS = 4
AM = 2
RW = 3
DS = 4


def kernel(
    chips, a_hbm, g_hbm, out, at, a_stage, g_buf, whole, own, d_send, d_recv, r_send, r_recv,
    a_sem, h_sem, g_sem, ds_sem, dr_sem, rs_sem, gs_sem, rr_sem, fs_sem, fr_sem,
):
    matrices, tokens, d = a_hbm.shape
    ff = g_hbm.shape[2]
    half = d // CORES
    per_matrix = ff // NB
    rounds = matrices * per_matrix // chips
    steps = rounds * chips
    per_wave = RW * chips
    waves = steps // per_wave
    forwards = per_wave - RW
    block = tokens // AS
    f32, bf16 = jnp.float32, jnp.bfloat16

    me = lax.axis_index("dp")
    chip, core = me // CORES, lax.rem(me, CORES)
    way = 1 - 2 * core
    peer = chip * CORES + 1 - core
    right = lax.rem(chip + way + chips, chips) * CORES + core
    left = lax.rem(chip - way + chips, chips) * CORES + core

    def rows(c):
        return pl.ds(pl.multiple_of(c * half, half), half)

    my_rows, peer_rows = rows(core), rows(1 - core)

    def nth(s):
        return lax.rem(chip - 1 + s + chips * chips, chips)

    def mine(j):
        return nth(-way * j)

    def peers(j):
        return nth(way * j)

    def split(i):
        w, ii = i // per_wave, lax.rem(i, per_wave)
        return ii // RW, w * RW + lax.rem(ii, RW)

    def place(r, ch):
        c = r * chips + ch
        return c // per_matrix, pl.ds(pl.multiple_of(lax.rem(c, per_matrix) * NB, NB), NB)

    def g_slot(r, ch):
        return lax.rem(r, RW) * chips + ch

    def tokens_of(b):
        return pl.ds(pl.multiple_of(b * block, block), block)

    def load_a(m, b):
        return pltpu.make_async_copy(a_hbm.at[m, tokens_of(b), :], a_stage.at[b], a_sem.at[b])

    def load_g(r, ch):
        n, cols = place(r, ch)
        slot = g_slot(r, ch)
        return pltpu.make_async_copy(g_hbm.at[n, :, cols], g_buf.at[slot], g_sem.at[slot])

    def load_first(b):
        n, cols = place(0, nth(0))
        return pltpu.make_async_copy(
            g_hbm.at[n, tokens_of(b), cols], g_buf.at[g_slot(0, nth(0)), tokens_of(b)], h_sem.at[b])

    def to(device, src, dst, send_sem, recv_sem):
        return pltpu.make_async_remote_copy(
            src_ref=src, dst_ref=dst, send_sem=send_sem, recv_sem=recv_sem,
            device_id={"dp": device}, device_id_type=MESH)

    def swap(i):
        s = lax.rem(i, DS)
        return to(peer, d_send.at[s], d_recv.at[s], ds_sem.at[s], dr_sem.at[s])

    def reduce_hop(r, j):
        k = r * (chips - 1) + j
        return to(right, r_send.at[k], r_recv.at[k], rs_sem.at[0], rr_sem.at[r * chips + j])

    def gather_hop(r, t, ch):
        n, cols = place(r, ch)
        at_ = out.at[n, my_rows, cols]
        return to(right, at_, at_, gs_sem.at[0], rr_sem.at[r * chips + lax.rem(t + chips - 1, chips)])

    def hand_over(r, ch):
        n, cols = place(r, ch)
        at_ = out.at[n, my_rows, cols]
        return to(peer, at_, at_, fs_sem.at[0], fr_sem.at[0])

    def transpose(m, b):
        load_a(m, b).wait()
        at[lax.rem(m, AM), :, tokens_of(b)] = a_stage[b].T

        if m % 2 == 0:
            load_a(m + 1, b).start()

    def dot(i, ch, which):
        j, r = split(i)
        m = (r * chips + ch) // per_matrix
        return jnp.dot(at[lax.rem(m, AM), which, :], g_buf[g_slot(r, ch)], preferred_element_type=f32)

    def combine(i):
        j, r = split(i)
        s = lax.rem(i, DS)
        swap(i).wait_recv()

        @pl.when(j == 0)
        def _():
            r_send[r * (chips - 1)] = (own[...] + d_recv[s].astype(f32)).astype(bf16)
            reduce_hop(r, 0).start()

        @pl.when(j > 0)
        def _():
            reduce_hop(r, j - 1).wait_recv()
            own[...] = own[...] + d_recv[s].astype(f32) + r_recv[r * (chips - 1) + j - 1].astype(f32)

        @pl.when((j > 0) & (j < chips - 1))
        def _():
            r_send[r * (chips - 1) + j] = own[...].astype(bf16)
            reduce_hop(r, j).start()

        @pl.when(j == chips - 1)
        def _():
            ch = mine(chips - 1)
            n, cols = place(r, ch)
            out[n, my_rows, cols] = own[...].astype(bf16)
            gather_hop(r, 0, ch).start()
            hand_over(r, ch).start()

    def forward(w, x):
        t, r = x // RW, w * RW + lax.rem(x, RW)
        ch = mine(t)
        gather_hop(r, t, ch).wait_recv()

        @pl.when(t < chips - 2)
        def _():
            gather_hop(r, t + 1, ch).start()

        hand_over(r, ch).start()

    def send_peers(i, value):
        d_send[lax.rem(i, DS)] = value.astype(bf16)

    first, last = {}, {}
    for j in range(chips):
        for s in sorted({j, -j % chips}):
            first.setdefault(s, j)
            last[s] = j

    for b in range(AS):
        load_a(0, b).start()
        load_first(b).start()

    barrier = pltpu.get_barrier_semaphore()
    for other in (left, right, peer):
        pl.semaphore_signal(barrier, inc=1, device_id={"dp": other}, device_id_type=MESH)

    always = chip >= 0

    def products(b):
        cols = slice(b * block, (b + 1) * block)
        term = jnp.dot(at[0, :, cols], g_buf[g_slot(0, nth(0)), cols, :], preferred_element_type=f32)
        whole[...] = whole[...] + term if b else term

    for b in range(AS + 1):
        m, k = b // AS, b % AS
        load_a(m, k).wait()
        if b < AS:
            load_first(b).wait()

        @pl.when(always)
        def _():
            at[m, :, k * block:(k + 1) * block] = a_stage[k].T
            if b:
                products(b - 1)

        if b < AS:
            load_a(1, b).start()
        if b == AS - 1:
            load_g(1, nth(0)).start()

    send_peers(0, whole[peer_rows, :])
    own[...] = whole[my_rows, :]
    pl.semaphore_wait(barrier, 3)
    swap(0).start()

    for b in range(1, AS):
        load_a(1, b).wait()
        at[1, :, b * block:(b + 1) * block] = a_stage[b].T
        if b == AS - 2:
            load_g(2, nth(0)).start()

    combine(0)
    for j in range(1, chips):
        for r in range(RW):
            for s in first:
                if first[s] == j:
                    load_g(r, nth(s)).start()

    def lone_peers(i, r):
        load_g(r, nth(0)).wait()

        @pl.when(always)
        def _():
            send_peers(i, dot(i, peers(0), peer_rows))

        swap(i).start()

    def lone_mine(i):
        @pl.when(always)
        def _():
            own[...] = dot(i, mine(chips - 1), my_rows)

    def transpose_some(m, begin, end):
        def one(b, carry):
            transpose(m, b)
            return carry

        lax.fori_loop(begin, end, one, 0)

    lone_peers(1, 1)

    def step(i, carry):
        w, ii = i // per_wave, lax.rem(i, per_wave)
        j, r = split(i)
        nj, nr = split(i + 1)

        for jj in range(chips):
            new = [s for s in first if first[s] == jj]
            if new:
                @pl.when(nj == jj)
                def _():
                    for s in new:
                        load_g(nr, nth(s)).wait()

        @pl.when(i + 1 >= DS)
        def _():
            swap(i + 1 - DS).wait_send()

        own[...] = dot(i, mine(j), my_rows)
        send_peers(i + 1, dot(i + 1, peers(nj), peer_rows))
        swap(i + 1).start()
        combine(i)

        @pl.when((w > 0) & (ii < forwards - 3))
        def _():
            forward(w - 1, ii + 3)

        for jj in range(chips):
            free = [s for s in last if last[s] == jj > 0]
            if free:
                @pl.when((j == jj) & (r + RW < rounds))
                def _():
                    for s in free:
                        load_g(r + RW, nth(s)).start()

        return carry

    for w in range(waves):
        begin, end = w * per_wave, (w + 1) * per_wave

        if w:
            transpose_some(2 * w, 0, AS)
            forward(w - 1, 0)
            swap(begin - DS).wait_send()
            lone_peers(begin, w * RW)
            transpose_some(2 * w + 1, 0, AS // 2)
            forward(w - 1, 1)
            transpose_some(2 * w + 1, AS // 2, AS)
            forward(w - 1, 2)

        begin += w == 0
        if w + 1 < waves:
            middle = (begin + end) // 2
            lax.fori_loop(begin, middle, step, 0)
            for b in range(AS):
                load_a(2 * w + 2, b).start()
            for r in range(RW):
                load_g((w + 1) * RW + r, nth(0)).start()
            begin = middle
        lax.fori_loop(begin, end - 1, step, 0)
        lone_mine(end - 1)
        combine(end - 1)
        if w + 1 < waves:
            for q in last:
                if last[q] == chips - 1:
                    load_g((w + 2) * RW - 1, nth(q)).start()

    def rest(x, carry):
        forward(waves - 1, x)
        return carry

    lax.fori_loop(0, forwards, rest, 0)

    for i in range(steps - DS, steps):
        swap(i).wait_send()
    to(right, r_send, r_recv, rs_sem.at[0], rr_sem.at[0]).wait_send()
    to(right, r_send, r_recv, gs_sem.at[0], rr_sem.at[0]).wait_send()
    all_mine = out.at[:, my_rows, :]
    to(peer, all_mine, all_mine, fs_sem.at[0], fr_sem.at[0]).wait()


def solution(mesh):
    chips = mesh.shape["dp"] // CORES

    def one(a, g):
        a, g = a[0], g[0]
        matrices, tokens, d = a.shape
        ff = g.shape[2]
        half = d // CORES
        rounds = matrices * ff // NB // chips
        hops = rounds * (chips - 1)
        bf16, f32 = jnp.bfloat16, jnp.float32
        sems = [AS, AS, RW * chips, DS, DS, 1, 1, rounds * chips, 1, 1]
        return pl.pallas_call(
            functools.partial(kernel, chips),
            out_shape=pltpu.MemorySpace.VMEM((matrices, d, ff), bf16),
            in_specs=[pl.BlockSpec(memory_space=pltpu.MemorySpace.HBM)] * 2,
            out_specs=pl.BlockSpec(memory_space=pltpu.MemorySpace.VMEM),
            scratch_shapes=[
                pltpu.VMEM((AM, d, tokens), bf16),
                pltpu.VMEM((AS, tokens // AS, d), bf16),
                pltpu.VMEM((RW * chips, tokens, NB), bf16),
                pltpu.VMEM((d, NB), f32),
                pltpu.VMEM((half, NB), f32),
                pltpu.VMEM((DS, half, NB), bf16),
                pltpu.VMEM((DS, half, NB), bf16),
                pltpu.VMEM((hops, half, NB), bf16),
                pltpu.VMEM((hops, half, NB), bf16),
                *(pltpu.SemaphoreType.DMA((n,)) for n in sems),
            ],
            compiler_params=pltpu.CompilerParams(
                collective_id=0, has_side_effects=True, vmem_limit_bytes=54 * 2**20),
        )(a, g)

    return jax.shard_map(
        one, mesh=mesh, in_specs=(P(("rep", "dp")),) * 2, out_specs=P("rep"), check_vma=False)
```

```python
import functools

import jax
import jax.numpy as jnp
from jax import lax
from jax.experimental import pallas as pl
from jax.experimental.pallas import tpu as pltpu
from jax.sharding import PartitionSpec as P

MESH = pl.DeviceIdType.MESH
CORES = 2
NB = 256
AS = 4
AM = 2
RW = 3
DS = 4
NEAR = 240


def kernel(
    chips, a_hbm, g_hbm, out, at, a_stage, g_buf, whole, own, d_send, d_recv, r_send, r_recv,
    a_sem, h_sem, g_sem, ds_sem, dr_sem, rs_sem, gs_sem, rr_sem, xr_sem, fs_sem, fr_sem,
):
    matrices, tokens, d = a_hbm.shape
    ff = g_hbm.shape[2]
    half = d // CORES
    per_matrix = ff // NB
    rounds = matrices * per_matrix // chips
    steps = rounds * chips
    per_wave = RW * chips
    waves = steps // per_wave
    forwards = per_wave - RW
    block = tokens // AS
    f32, bf16 = jnp.float32, jnp.bfloat16

    me = lax.axis_index("dp")
    chip, core = me // CORES, lax.rem(me, CORES)
    way = 1 - 2 * core
    peer = chip * CORES + 1 - core
    right = lax.rem(chip + way + chips, chips) * CORES + core
    left = lax.rem(chip - way + chips, chips) * CORES + core

    def rows(c):
        return pl.ds(pl.multiple_of(c * half, half), half)

    my_rows, peer_rows = rows(core), rows(1 - core)

    def nth(s):
        return lax.rem(chip - 1 + s + chips * chips, chips)

    def mine(j):
        return nth(-way * j)

    def peers(j):
        return nth(way * j)

    def split(i):
        w, ii = i // per_wave, lax.rem(i, per_wave)
        return ii // RW, w * RW + lax.rem(ii, RW)

    def place(r, ch):
        c = r * chips + ch
        return c // per_matrix, pl.ds(pl.multiple_of(lax.rem(c, per_matrix) * NB, NB), NB)

    def g_slot(r, ch):
        return lax.rem(r, RW) * chips + ch

    def tokens_of(b):
        return pl.ds(pl.multiple_of(b * block, block), block)

    def load_a(m, b):
        return pltpu.make_async_copy(a_hbm.at[m, tokens_of(b), :], a_stage.at[b], a_sem.at[b])

    def load_g(r, ch):
        n, cols = place(r, ch)
        slot = g_slot(r, ch)
        return pltpu.make_async_copy(g_hbm.at[n, :, cols], g_buf.at[slot], g_sem.at[slot])

    def load_first(b):
        n, cols = place(0, nth(0))
        return pltpu.make_async_copy(
            g_hbm.at[n, tokens_of(b), cols], g_buf.at[g_slot(0, nth(0)), tokens_of(b)], h_sem.at[b])

    def to(device, src, dst, send_sem, recv_sem):
        return pltpu.make_async_remote_copy(
            src_ref=src, dst_ref=dst, send_sem=send_sem, recv_sem=recv_sem,
            device_id={"dp": device}, device_id_type=MESH)

    def swap(i):
        s = lax.rem(i, DS)
        return to(peer, d_send.at[s], d_recv.at[s], ds_sem.at[s], dr_sem.at[s])

    def reduce_hop(r, j):
        k = r * (chips - 1) + j
        return to(right, r_send.at[k], r_recv.at[k], rs_sem.at[0], rr_sem.at[r * chips + j])

    def gather_hop(r, t, ch):
        n, cols = place(r, ch)
        at_ = out.at[n, my_rows, cols]
        return to(right, at_, at_, gs_sem.at[0], rr_sem.at[r * chips + lax.rem(t + chips - 1, chips)])

    final, longer = rounds - 1, core == 0

    def near(ch):
        n, cols = place(final, ch)
        at_ = out.at[n, pl.ds(pl.multiple_of(core * half, half), NEAR), cols]
        return to(left, at_, at_, gs_sem.at[0], xr_sem.at[0])

    def final_hop(ch):
        n, cols = place(final, ch)
        at_ = out.at[n, pl.ds(pl.multiple_of(core * half + NEAR, 16), half - NEAR), cols]
        return to(right, at_, at_, gs_sem.at[0], rr_sem.at[final * chips + chips - 3])

    def hand_over(r, ch):
        n, cols = place(r, ch)
        at_ = out.at[n, my_rows, cols]
        return to(peer, at_, at_, fs_sem.at[0], fr_sem.at[0])

    def transpose(m, b):
        load_a(m, b).wait()
        at[lax.rem(m, AM), :, tokens_of(b)] = a_stage[b].T

        if m % 2 == 0:
            load_a(m + 1, b).start()

    def dot(i, ch, which):
        j, r = split(i)
        m = (r * chips + ch) // per_matrix
        return jnp.dot(at[lax.rem(m, AM), which, :], g_buf[g_slot(r, ch)], preferred_element_type=f32)

    def combine(i):
        j, r = split(i)
        s = lax.rem(i, DS)
        swap(i).wait_recv()

        @pl.when(j == 0)
        def _():
            r_send[r * (chips - 1)] = (own[...] + d_recv[s].astype(f32)).astype(bf16)
            reduce_hop(r, 0).start()

        @pl.when(j > 0)
        def _():
            reduce_hop(r, j - 1).wait_recv()
            own[...] = own[...] + d_recv[s].astype(f32) + r_recv[r * (chips - 1) + j - 1].astype(f32)

        @pl.when((j > 0) & (j < chips - 1))
        def _():
            r_send[r * (chips - 1) + j] = own[...].astype(bf16)
            reduce_hop(r, j).start()

        @pl.when(j == chips - 1)
        def _():
            ch = mine(chips - 1)
            n, cols = place(r, ch)
            out[n, my_rows, cols] = own[...].astype(bf16)
            gather_hop(r, 0, ch).start()
            hand_over(r, ch).start()

            @pl.when((r == final) & longer)
            def _():
                near(ch).start()

    def forward(w, x, parted=False):
        t, r = x // RW, w * RW + lax.rem(x, RW)
        ch = mine(t)
        gather_hop(r, t, ch).wait_recv()

        @pl.when((t < chips - 2) & jnp.logical_not(parted))
        def _():
            gather_hop(r, t + 1, ch).start()

        if parted is not False:
            @pl.when(parted)
            def _():
                final_hop(ch).start()

        hand_over(r, ch).start()

    def send_peers(i, value):
        d_send[lax.rem(i, DS)] = value.astype(bf16)

    first, last = {}, {}
    for j in range(chips):
        for s in sorted({j, -j % chips}):
            first.setdefault(s, j)
            last[s] = j

    for b in range(AS):
        load_a(0, b).start()
        load_first(b).start()

    barrier = pltpu.get_barrier_semaphore()
    for other in (left, right, peer):
        pl.semaphore_signal(barrier, inc=1, device_id={"dp": other}, device_id_type=MESH)

    always = chip >= 0

    def products(b):
        cols = slice(b * block, (b + 1) * block)
        term = jnp.dot(at[0, :, cols], g_buf[g_slot(0, nth(0)), cols, :], preferred_element_type=f32)
        whole[...] = whole[...] + term if b else term

    for b in range(AS + 1):
        m, k = b // AS, b % AS
        load_a(m, k).wait()
        if b < AS:
            load_first(b).wait()

        @pl.when(always)
        def _():
            at[m, :, k * block:(k + 1) * block] = a_stage[k].T
            if b:
                products(b - 1)

        if b < AS:
            load_a(1, b).start()
        if b == AS - 1:
            load_g(1, nth(0)).start()

    send_peers(0, whole[peer_rows, :])
    own[...] = whole[my_rows, :]
    pl.semaphore_wait(barrier, 3)
    swap(0).start()

    for b in range(1, AS):
        load_a(1, b).wait()
        at[1, :, b * block:(b + 1) * block] = a_stage[b].T
        if b == AS - 2:
            load_g(2, nth(0)).start()

    combine(0)
    for j in range(1, chips):
        for r in range(RW):
            for s in first:
                if first[s] == j:
                    load_g(r, nth(s)).start()

    def lone_peers(i, r):
        load_g(r, nth(0)).wait()

        @pl.when(always)
        def _():
            send_peers(i, dot(i, peers(0), peer_rows))

        swap(i).start()

    def lone_mine(i):
        @pl.when(always)
        def _():
            own[...] = dot(i, mine(chips - 1), my_rows)

    def transpose_some(m, begin, end):
        def one(b, carry):
            transpose(m, b)
            return carry

        lax.fori_loop(begin, end, one, 0)

    lone_peers(1, 1)

    def step(i, carry):
        w, ii = i // per_wave, lax.rem(i, per_wave)
        j, r = split(i)
        nj, nr = split(i + 1)

        for jj in range(chips):
            new = [s for s in first if first[s] == jj]
            if new:
                @pl.when(nj == jj)
                def _():
                    for s in new:
                        load_g(nr, nth(s)).wait()

        @pl.when(i + 1 >= DS)
        def _():
            swap(i + 1 - DS).wait_send()

        own[...] = dot(i, mine(j), my_rows)
        send_peers(i + 1, dot(i + 1, peers(nj), peer_rows))
        swap(i + 1).start()
        combine(i)

        @pl.when((w > 0) & (ii < forwards - 3))
        def _():
            forward(w - 1, ii + 3)

        for jj in range(chips):
            free = [s for s in last if last[s] == jj > 0]
            if free:
                @pl.when((j == jj) & (r + RW < rounds))
                def _():
                    for s in free:
                        load_g(r + RW, nth(s)).start()

        return carry

    for w in range(waves):
        begin, end = w * per_wave, (w + 1) * per_wave

        if w:
            transpose_some(2 * w, 0, AS)
            forward(w - 1, 0)
            swap(begin - DS).wait_send()
            lone_peers(begin, w * RW)
            transpose_some(2 * w + 1, 0, AS // 2)
            forward(w - 1, 1)
            transpose_some(2 * w + 1, AS // 2, AS)
            forward(w - 1, 2)

        begin += w == 0
        if w + 1 < waves:
            middle = (begin + end) // 2
            lax.fori_loop(begin, middle, step, 0)
            for b in range(AS):
                load_a(2 * w + 2, b).start()
            for r in range(RW):
                load_g((w + 1) * RW + r, nth(0)).start()
            begin = middle
        lax.fori_loop(begin, end - 1, step, 0)
        lone_mine(end - 1)
        combine(end - 1)
        if w + 1 < waves:
            for q in last:
                if last[q] == chips - 1:
                    load_g((w + 2) * RW - 1, nth(q)).start()

    def rest(x, carry):
        forward(waves - 1, x, (x == forwards - RW - 1) & longer)
        return carry

    lax.fori_loop(0, forwards - 1, rest, 0)
    ch = mine(chips - 2)

    @pl.when(longer)
    def _():
        near(ch).wait_recv()
        final_hop(ch).wait_recv()

    @pl.when(jnp.logical_not(longer))
    def _():
        gather_hop(final, chips - 2, ch).wait_recv()

    hand_over(final, ch).start()

    for i in range(steps - DS, steps):
        swap(i).wait_send()
    to(right, r_send, r_recv, rs_sem.at[0], rr_sem.at[0]).wait_send()
    to(right, r_send, r_recv, gs_sem.at[0], rr_sem.at[0]).wait_send()
    all_mine = out.at[:, my_rows, :]
    to(peer, all_mine, all_mine, fs_sem.at[0], fr_sem.at[0]).wait()


def solution(mesh):
    chips = mesh.shape["dp"] // CORES

    def one(a, g):
        a, g = a[0], g[0]
        matrices, tokens, d = a.shape
        ff = g.shape[2]
        half = d // CORES
        rounds = matrices * ff // NB // chips
        hops = rounds * (chips - 1)
        bf16, f32 = jnp.bfloat16, jnp.float32
        sems = [AS, AS, RW * chips, DS, DS, 1, 1, rounds * chips, 1, 1, 1]
        return pl.pallas_call(
            functools.partial(kernel, chips),
            out_shape=pltpu.MemorySpace.VMEM((matrices, d, ff), bf16),
            in_specs=[pl.BlockSpec(memory_space=pltpu.MemorySpace.HBM)] * 2,
            out_specs=pl.BlockSpec(memory_space=pltpu.MemorySpace.VMEM),
            scratch_shapes=[
                pltpu.VMEM((AM, d, tokens), bf16),
                pltpu.VMEM((AS, tokens // AS, d), bf16),
                pltpu.VMEM((RW * chips, tokens, NB), bf16),
                pltpu.VMEM((d, NB), f32),
                pltpu.VMEM((half, NB), f32),
                pltpu.VMEM((DS, half, NB), bf16),
                pltpu.VMEM((DS, half, NB), bf16),
                pltpu.VMEM((hops, half, NB), bf16),
                pltpu.VMEM((hops, half, NB), bf16),
                *(pltpu.SemaphoreType.DMA((n,)) for n in sems),
            ],
            compiler_params=pltpu.CompilerParams(
                collective_id=0, has_side_effects=True, vmem_limit_bytes=54 * 2**20),
        )(a, g)

    return jax.shard_map(
        one, mesh=mesh, in_specs=(P(("rep", "dp")),) * 2, out_specs=P("rep"), check_vma=False)
```
